128 devices in a mesh: ma: 16 (over x, y), lev: 8 (over z, core).
Axes of the slice: x: 4, y: 4, z: 4, core: 2. Of those that a mesh axis runs over, the one named last changes fastest.
Arguments:
- spectral_state: float32 [1280, 2, 32, 1280], P('ma', None, None, 'lev'), may hold values from -6 to 6
- forcing_noise: bfloat16 [1280, 2, 32, 1280], P('ma', None, None, 'lev'), may hold values from -6 to 6
- decay_rate: float32 [32], replicated, may hold values from 0.3 to 0.95
- amplitude: float32 [1280], P('lev'), may hold values from 0.2 to 2
- legendre: bfloat16 [1280, 1280, 640], P('ma', 'lev'), may hold values from -0.0048828125 to 0.0048828125
- wave_of_slot: int32 [1280], replicated, may hold values from 0 to 1279, each once
- lat_of_row: int32 [1280], replicated, may hold values from 0 to 1279, each once
Outputs:
- new_state: float32 [1280, 2, 32, 1280], P('ma', None, None, 'lev')
- pattern: bfloat16 [32, 1280, 2560], P('lev', 'ma')
The draws below stay inside these ranges and needn't reach their ends.
Inputs may be any that keep to these rules, and one draw needn't show every extreme that they name: `wave_of_slot`: each zonal wavenumber is held by exactly one slot. `lat_of_row`: each latitude is held by exactly one row.
All inputs are finite; a program needn't handle non-finite values.
Results may differ from the reference program's by a relative error of at most 0.014.
Values may be sent and summed in bfloat16 or wider, within the bound.
A program may use at most 192 MiB of HBM per device.

```python
import math
import jax
import jax.numpy as jnp
from jax import lax

M = 1280
N = 1280
NLAT = 1280
NLON = 2560
LEVELS = 32
N_LEV = 8


def levels(own_key, dims, pieces, smallest, top_value):
    level = 1.0
    for axis_at, parts in pieces:
        draws = jax.random.uniform(jax.random.fold_in(jax.random.fold_in(own_key, 6), axis_at), (parts,), jnp.float32, smallest / len(pieces), top_value / len(pieces))
        level = level * jnp.repeat(jnp.exp(draws), dims[axis_at] // parts).reshape((-1,) + (1,) * (len(dims) - 1 - axis_at))
    return level


def normal_values(stream_key, shape, spread, most, cuts=(), kind=jnp.bfloat16):
    array = spread * jax.random.normal(stream_key, shape, jnp.float32)
    if cuts:
        array = array * levels(stream_key, shape, cuts, -0.22, 0.18)
    return jnp.clip(array, -most, most).astype(kind)


def setup_inputs(seed: int = 0) -> dict:
    key_list = jax.random.split(jax.random.key(seed), 8)
    return {
        "spectral_state": normal_values(key_list[0], (M, 2, LEVELS, N), 1.0, 6.0, ((0, 16), (3, 8)), jnp.float32),
        "forcing_noise": normal_values(key_list[1], (M, 2, LEVELS, N), 1.0, 6.0, ((0, 16), (3, 8))),
        "decay_rate": jnp.clip(jnp.exp(jax.random.uniform(key_list[2], (LEVELS,), jnp.float32, math.log(0.3), math.log(0.95))), 0.3, 0.95),
        "amplitude": jnp.clip(jnp.exp(math.log(2.0) - 2.3025851 * jax.random.uniform(key_list[3], (N,), jnp.float32) ** levels(key_list[3], (N,), ((0, 8),), -0.2, 0.2)), 0.2, 2.0),
        "legendre": normal_values(key_list[4], (M, N, NLAT // 2), (N * M) ** -0.5, 0.0048828125, ((0, 16), (1, 8))),
        "wave_of_slot": jax.random.permutation(key_list[5], M).astype(jnp.int32),
        "lat_of_row": jax.random.permutation(key_list[6], NLAT).astype(jnp.int32),
    }


def build_table(wavenum, width):
    column = jnp.arange(width, dtype=jnp.int32)
    product = (wavenum[:, None] * column[None, :]) % width
    phase_angle = product.astype(jnp.float32) * jnp.float32(2.0 * math.pi / width)
    factor = jnp.where(wavenum == 0, jnp.float32(1.0), jnp.float32(2.0))[:, None]
    stacked = jnp.stack([factor * jnp.cos(phase_angle), -factor * jnp.sin(phase_angle)], axis=1)
    return stacked.astype(jnp.bfloat16)


def reference(spectral_state, forcing_noise, decay_rate, amplitude, legendre, wave_of_slot, lat_of_row):
    wavenum = wave_of_slot.astype(jnp.int32)
    total_n = jnp.arange(N, dtype=jnp.int32)
    valid_mask = total_n[None, :] >= wavenum[:, None]
    updated = decay_rate[None, None, :, None] * spectral_state + amplitude[None, None, None, :] * forcing_noise.astype(jnp.float32)
    new_state = jnp.where(valid_mask[:, None, None, :], updated, jnp.float32(0.0))
    spectral = new_state.astype(jnp.bfloat16)
    odd_mask = ((total_n[None, :] - wavenum[:, None]) % 2) == 1
    block_len = N // N_LEV
    running = jnp.zeros((M, 2 * LEVELS, NLAT), jnp.float32)
    for block_index in range(N_LEV):
        lower = block_index * block_len
        piece = spectral[:, :, :, lower:lower + block_len].reshape(M, 2 * LEVELS, block_len)
        odd_block = odd_mask[:, None, lower:lower + block_len]
        even_part = jnp.where(odd_block, jnp.zeros_like(piece), piece)
        odd_part = jnp.where(odd_block, piece, jnp.zeros_like(piece))
        stacked = jnp.concatenate([even_part, odd_part], axis=1).astype(jnp.float32)
        weights = legendre[:, lower:lower + block_len, :].astype(jnp.float32)
        halves = jnp.einsum("scn,snj->scj", stacked, weights)
        even_sum = halves[:, :2 * LEVELS]
        odd_sum = halves[:, 2 * LEVELS:]
        full = jnp.concatenate([even_sum + odd_sum, jnp.flip(even_sum - odd_sum, axis=2)], axis=2)
        rounded = lax.optimization_barrier(full.astype(jnp.bfloat16))
        running = running + rounded.astype(jnp.float32)
    fourier = running.reshape(M, 2, LEVELS, NLAT).astype(jnp.bfloat16)
    by_row = jnp.take(fourier, lat_of_row.astype(jnp.int32), axis=3)
    dft_table = build_table(wavenum, NLON)
    pattern = jnp.einsum("srlk,srx->lkx", by_row.astype(jnp.float32), dft_table.astype(jnp.float32))
    return new_state, pattern.astype(jnp.bfloat16)
```

```python
import functools
import math

import jax
import jax.numpy as jnp
from jax import lax
from jax.experimental import pallas as pl
from jax.experimental.pallas import tpu as pltpu
from jax.sharding import PartitionSpec as P

NLON = 2560
S = 16
RP = 128
MESH = pl.DeviceIdType.MESH
F32 = jnp.float32
BF16 = jnp.bfloat16


def cos_of(v):
    turns = jnp.round(v * F32(1.0 / NLON))
    y = (v - turns * F32(NLON)) * F32(2.0 * math.pi / NLON)
    y2 = y * y
    acc = jnp.full_like(y2, 1.0 / math.factorial(16))
    for k in range(7, -1, -1):
        acc = acc * y2 + F32((-1.0) ** k / math.factorial(2 * k))
    return acc


def column_of(row):
    n = row.shape[1]
    eye = lax.broadcasted_iota(jnp.int32, (n, n), 0) == lax.broadcasted_iota(jnp.int32, (n, n), 1)
    return jnp.sum(jnp.where(eye, jnp.broadcast_to(row, (n, n)), F32(0.0)), axis=1, keepdims=True)


def transform_kernel(
    wave_s, wave_v, lat_v, decay_v, amp_v, st_h, nz_h, lg_h,
    f_out, t_out,
    stb, nzb, lgb, hv, pr, u1, ud, u2, d1, dd, d2, xf, xb, g, gb, tb, mcol,
    ld_sem, dd_s, dd_r, ring_s, ring_r, a2a_s, a2a_r, t_sem,
):
    zn, ns, rows, jn = hv.shape
    ma_n = gb.shape[2]
    nc = ns // S
    levels = stb.shape[3]
    wn = stb.shape[4]
    h = S // 2
    q = S // 4
    me_ma = lax.axis_index("ma")
    me_lev = lax.axis_index("lev")
    z = me_lev // 2
    core = me_lev % 2
    partner = z * 2 + 1 - core
    zu = lax.rem(z + 1, zn)
    zd = lax.rem(z + zn - 1, zn)
    zo = lax.rem(z + 2, zn)
    up = zu * 2 + core
    down = zd * 2 + core

    def load(c):
        b = c % 2
        return [
            pltpu.make_async_copy(st_h.at[pl.ds(c * S, S)], stb.at[b], ld_sem.at[b, 0]),
            pltpu.make_async_copy(nz_h.at[pl.ds(c * S, S)], nzb.at[b], ld_sem.at[b, 1]),
            pltpu.make_async_copy(lg_h.at[pl.ds(c * S, S)], lgb.at[b], ld_sem.at[b, 2]),
        ]

    for c in range(min(2, nc)):
        for cp in load(c):
            cp.start()

    barrier = pltpu.get_barrier_semaphore()
    for lev in (partner, up, down):
        pl.semaphore_signal(barrier, inc=1, device_id={"lev": lev}, device_id_type=MESH)

    def greet(o, carry):
        peer = lax.rem(me_ma + o, ma_n)
        pl.semaphore_signal(barrier, inc=1, device_id={"ma": peer}, device_id_type=MESH)
        pl.semaphore_signal(
            barrier, inc=1, device_id={"ma": peer, "lev": partner}, device_id_type=MESH
        )
        return carry

    lax.fori_loop(1, ma_n, greet, 0)

    dec = jnp.broadcast_to(column_of(decay_v[...]), (levels, wn))
    amp = amp_v[...]
    n_at = me_lev * wn + lax.broadcasted_iota(jnp.int32, (1, 1, wn), 2)
    mcol[...] = jnp.transpose(jnp.broadcast_to(wave_v[...].astype(F32), (8, wave_v.shape[1])))

    def compute(c):
        b = c % 2

        def slot(i, carry):
            m = wave_s[me_ma * ns + c * S + i]
            x = dec[None] * stb[b, i] + amp[None] * nzb[b, i].astype(F32)
            x = jnp.where(n_at >= m, x, F32(0.0)).reshape(2, zn, 8, wn)
            odd = (((n_at - m) & 1) == 1).reshape(1, 1, 1, wn)
            even_part = jnp.where(odd, F32(0.0), x)
            odd_part = jnp.where(odd, x, F32(0.0))
            lhs = jnp.concatenate([even_part, odd_part], axis=2).astype(BF16)
            lhs = lhs.reshape(2 * zn * 16, wn)
            out = jnp.dot(lhs, lgb[b, i], preferred_element_type=F32).astype(BF16)
            for p in range(2):
                for t in range(zn):
                    at = (p * zn + t) * 16
                    hv[t, c * S + i, p * 16 : (p + 1) * 16, :] = out[at : at + 16]
            return carry

        lax.fori_loop(0, S, slot, 0)

    def swap(c):
        return pltpu.make_async_remote_copy(
            src_ref=hv.at[:, pl.ds(c * S + (1 - core) * h, h)],
            dst_ref=pr.at[:, pl.ds(c * h, h)],
            send_sem=dd_s.at[c],
            recv_sem=dd_r.at[c],
            device_id={"lev": partner},
            device_id_type=MESH,
        )

    def hop(c, kind):
        up_to = kind < 3
        box = (u1, ud, u2, d1, dd, d2)[kind]
        plane = (zo, zu, zu, zo, zd, zd)[kind]
        half = (0, 1, 0, 1, 0, 1)[kind]
        return pltpu.make_async_remote_copy(
            src_ref=pr.at[plane, pl.ds(c * h + half * q, q)],
            dst_ref=box.at[pl.ds(c * q, q)],
            send_sem=ring_s.at[c, kind],
            recv_sem=ring_r.at[c, kind],
            device_id={"lev": up if up_to else down},
            device_id_type=MESH,
        )

    def merge(c, plane, first, count, more=None):
        def one(i, carry):
            at = c * h + first + i
            total = hv[plane, c * S + core * h + first + i].astype(F32) + pr[plane, at].astype(F32)
            if more is not None:
                total = total + more[c * q + i].astype(F32)
            pr[plane, at] = total.astype(BF16)
            return carry

        lax.fori_loop(0, count, one, 0)

    def far(c):
        swap(c).wait_recv()
        merge(c, zo, 0, h)
        hop(c, 0).start()
        hop(c, 3).start()

    def near(c):
        merge(c, zu, q, q)
        hop(c, 1).start()
        merge(c, zd, 0, q)
        hop(c, 4).start()

    def relay(c):
        hop(c, 0).wait_recv()
        merge(c, zu, 0, q, u1)
        hop(c, 2).start()
        hop(c, 3).wait_recv()
        merge(c, zd, q, q, d1)
        hop(c, 5).start()

    def finish(c):
        for kind in (1, 2, 4, 5):
            hop(c, kind).wait_recv()
        for half, (r1, r2) in enumerate(((u2, dd), (d2, ud))):

            def one(i, carry):
                at = half * q + i
                total = hv[z, c * S + core * h + at].astype(F32) + pr[z, c * h + at].astype(F32)
                total = total + (r1[c * q + i].astype(F32) + r2[c * q + i].astype(F32))
                for k in range(jn // 128):
                    at_row = pl.ds(pl.multiple_of(at * rows, rows), rows)
                    xf[k, at_row, :] = total[:, k * 128 : (k + 1) * 128]
                return carry

            lax.fori_loop(0, q, one, 0)
        for level in range(8):
            for k in range(jn // 128):
                north = []
                south = []
                for p in range(2):
                    even = xf[k, pl.ds(p * 16 + level, h, stride=rows), :]
                    odd = xf[k, pl.ds(p * 16 + 8 + level, h, stride=rows), :]
                    north.append(even + odd)
                    south.append(even - odd)
                at_row = slice(level * 16, (level + 1) * 16)
                at = k * 128
                xb[at_row, at : at + 128] = jnp.concatenate(north, axis=0).astype(BF16)
                xb[at_row, jn + at : jn + at + 128] = jnp.concatenate(south, axis=0).astype(BF16)

        def pick(m2, carry):
            out = jnp.dot(xb[...], g[m2], preferred_element_type=F32).astype(BF16)
            for tc in range(2):
                for k in range(2):
                    part = out[tc * 64 : (tc + 1) * 64, k * RP : (k + 1) * RP]
                    gb[c, tc, m2 * 2 + k] = part.reshape(4, 16, RP)
            return carry

        lax.fori_loop(0, ma_n // 2, pick, 0)
        place = pl.ds(pl.multiple_of((me_ma * 2 + core) * 16, 16), 16)

        def send(o, tc_flip):
            peer = lax.rem(me_ma + o, ma_n)
            tc = lax.rem(core + tc_flip, 2)
            pltpu.make_async_remote_copy(
                src_ref=gb.at[c, tc, peer],
                dst_ref=f_out.at[c, :, place, :],
                send_sem=a2a_s,
                recv_sem=a2a_r,
                device_id={"ma": peer, "lev": z * 2 + tc},
                device_id_type=MESH,
            ).start()

        def send_both(o, carry):
            send(o, 0)
            send(o, 1)
            return carry

        send(0, 1)
        lax.fori_loop(1, ma_n, send_both, 0)
        pltpu.make_async_copy(gb.at[c, core, me_ma], f_out.at[c, :, place, :], a2a_r).start()

    def selection():
        step = 128
        lane = (2 * RP,)

        def one(m2, carry):
            lat = lat_v[m2]
            for r0 in range(0, 2 * jn, step):
                k = r0 + lax.broadcasted_iota(jnp.int32, (step,) + lane, 0)
                k = k if r0 < jn else 3 * jn - 1 - k
                g[m2, r0 : r0 + step, :] = jnp.where(lat == k, F32(1.0), F32(0.0)).astype(BF16)
            return carry

        lax.fori_loop(0, ma_n // 2, one, 0)

    groups = tb.shape[0] // 16
    per = groups // nc

    def table(c):
        def one(i, carry):
            block = c * per + i
            src = (block % (2 * ma_n)) // 2
            first = src * ns + (block // (2 * ma_n)) * S + (block % 2) * h
            m = mcol[pl.ds(pl.multiple_of(first, 8), 8), 0:1]
            x = lax.broadcasted_iota(jnp.int32, (8, tb.shape[1]), 1).astype(F32)
            v = jnp.broadcast_to(m, (8, tb.shape[1])) * x
            w = jnp.broadcast_to(jnp.where(m == F32(0.0), F32(1.0), F32(2.0)), v.shape)
            both = jnp.concatenate([w * cos_of(v), w * cos_of(v + F32(NLON // 4))], axis=0)
            tb[pl.ds(pl.multiple_of(block * 16, 16), 16), :] = both.astype(BF16)
            return carry

        lax.fori_loop(0, per, one, 0)
        store_table(c).start()

    def store_table(c):
        part = pl.ds(c * per * 16, per * 16)
        return pltpu.make_async_copy(tb.at[part], t_out.at[part], t_sem.at[c])

    def stage(c):
        for cp in load(c):
            cp.wait()
        compute(c)
        if c + 2 < nc:
            for cp in load(c + 2):
                cp.start()
        if c == 0:
            pl.semaphore_wait(barrier, 3 + 2 * (ma_n - 1))
        swap(c).start()

    stage(0)
    stage(1)
    far(0)
    far(1)
    near(0)
    for c in range(2, nc):
        stage(c)
        if c < nc - 1:
            relay(c - 2)
            far(c)
            near(c - 1)
    selection()
    last = nc - 1
    if nc > 2:
        relay(last - 2)
        far(last)
        near(last - 1)
        finish(0)
        table(0)
        for c in range(1, nc - 1):
            if c < nc - 2:
                finish(c)
            table(c)
            if c == nc - 3:
                relay(last - 1)
                near(last)
        if nc == 3:
            relay(last - 1)
            near(last)
        table(nc - 1)
        relay(last)
        finish(nc - 2)
        finish(nc - 1)
    else:
        relay(0)
        near(1)
        table(0)
        relay(1)
        table(1)
        finish(0)
        finish(1)

    for c in range(nc):
        swap(c).wait_send()
        for kind in range(6):
            hop(c, kind).wait_send()
        store_table(c).wait()
    pltpu.make_async_copy(f_out, f_out, a2a_r).wait()
    sent = gb_flat(gb, nc * (2 * ma_n - 1))
    pltpu.make_async_copy(sent, sent, a2a_s).wait()


def gb_flat(gb, count):
    flat = gb.reshape(gb.shape[0] * gb.shape[1] * gb.shape[2], 4, 16, RP)
    return flat.at[pl.ds(0, count)]


def grid_kernel(wave_s, f, sign, t, st, nz, decay_v, amp_v, new_state, out, lhs):
    step = pl.program_id(0)
    nc, ln, kc, _ = f.shape
    rb = out.shape[1]
    half = out.shape[2] // 2
    xb = t.shape[1]

    @pl.when(step == 0)
    def _():
        for c in range(nc):
            for level in range(ln):
                block = jnp.transpose(f[c, level])[:rb]
                at = slice(c * kc, (c + 1) * kc)
                lhs[level * rb : (level + 1) * rb, at] = block
                lhs[(ln + level) * rb : (ln + level + 1) * rb, at] = block * sign[:, at]

    levels = st.shape[2]
    wn = st.shape[3]
    dec = jnp.broadcast_to(column_of(decay_v[...]), (levels, wn))
    amp = amp_v[...]
    n_at = lax.axis_index("lev") * wn + lax.broadcasted_iota(jnp.int32, (1, 1, wn), 2)
    first = lax.axis_index("ma") * (st.shape[0] * pl.num_programs(0)) + step * st.shape[0]

    def slot(i, carry):
        m = wave_s[first + i]
        x = dec[None] * st[i] + amp[None] * nz[i].astype(F32)
        new_state[i] = jnp.where(n_at >= m, x, F32(0.0))
        return carry

    lax.fori_loop(0, st.shape[0], slot, 0)
    for k in range(2):
        for level in range(ln):
            r0 = (k * ln + level) * rb
            part = jnp.dot(lhs[r0 : r0 + rb, :], t[...], preferred_element_type=F32)
            at = pl.ds(pl.multiple_of(k * half + step * xb, 128), xb)
            out[level, :, at] = part.astype(BF16)


def body(spectral_state, forcing_noise, decay_rate, amplitude, legendre, wave_of_slot, lat_of_row):
    ns, _, levels, wn = spectral_state.shape
    jn = legendre.shape[2]
    nlat = lat_of_row.shape[0]
    mn = wave_of_slot.shape[0]
    ma_n = mn // ns
    lev_n = lax.axis_size("lev")
    zn = lev_n // 2
    ln = levels // lev_n
    rb = nlat // ma_n
    nc = ns // S
    kn = 2 * mn
    half = NLON // 2
    wave_row = wave_of_slot.reshape(1, mn)
    lat_rows = jnp.pad(lat_of_row.reshape(ma_n, rb), ((0, 0), (0, RP - rb)), constant_values=-1)
    lat_rows = lat_rows.reshape(ma_n // 2, 1, 2 * RP)
    decay_row = decay_rate.reshape(1, levels)
    amp_row = amplitude.reshape(1, wn)
    sign = (1 - 2 * (wave_of_slot % 2)).astype(BF16).reshape(ma_n, nc, 2, 1, S // 2)
    sign = jnp.broadcast_to(sign.transpose(1, 0, 2, 3, 4), (nc, ma_n, 2, 2, S // 2))
    sign = sign.reshape(1, kn)

    smem = pl.BlockSpec(memory_space=pltpu.SMEM)
    vmem = pl.BlockSpec(memory_space=pltpu.VMEM)
    hbm = pl.BlockSpec(memory_space=pl.ANY)
    box = pltpu.VMEM((nc * S // 4, 32, jn), BF16)
    f, t = pl.pallas_call(
        transform_kernel,
        out_shape=(
            jax.ShapeDtypeStruct((nc, ln, ma_n * 2 * 16, RP), BF16),
            jax.ShapeDtypeStruct((kn, half), BF16),
        ),
        in_specs=[smem, vmem, vmem, vmem, vmem, hbm, hbm, hbm],
        out_specs=(hbm, hbm),
        scratch_shapes=[
            pltpu.VMEM((2, S, 2, levels, wn), F32),
            pltpu.VMEM((2, S, 2, levels, wn), BF16),
            pltpu.VMEM((2, S, wn, jn), BF16),
            pltpu.VMEM((zn, ns, 32, jn), BF16),
            pltpu.VMEM((zn, ns // 2, 32, jn), BF16),
            box, box, box, box, box, box,
            pltpu.VMEM((jn // 128, S // 2 * 32, 128), F32),
            pltpu.VMEM((128, 2 * jn), BF16),
            pltpu.VMEM((ma_n // 2, 2 * jn, 2 * RP), BF16),
            pltpu.VMEM((nc, 2, ma_n, 4, 16, RP), BF16),
            pltpu.VMEM((kn, half), BF16),
            pltpu.VMEM((mn, 8), F32),
            pltpu.SemaphoreType.DMA((2, 3)),
            pltpu.SemaphoreType.DMA((nc,)),
            pltpu.SemaphoreType.DMA((nc,)),
            pltpu.SemaphoreType.DMA((nc, 6)),
            pltpu.SemaphoreType.DMA((nc, 6)),
            pltpu.SemaphoreType.DMA,
            pltpu.SemaphoreType.DMA,
            pltpu.SemaphoreType.DMA((nc,)),
        ],
        compiler_params=pltpu.CompilerParams(
            collective_id=0, has_side_effects=True, vmem_limit_bytes=66_000_000
        ),
        name="transform",
    )(wave_of_slot, wave_row, lat_rows, decay_row, amp_row, spectral_state, forcing_noise, legendre)

    steps = nc
    sb = ns // steps
    xb = half // steps
    new_state, pattern = pl.pallas_call(
        grid_kernel,
        grid=(steps,),
        out_shape=(
            jax.ShapeDtypeStruct((ns, 2, levels, wn), F32),
            jax.ShapeDtypeStruct((ln, rb, NLON), BF16),
        ),
        in_specs=[
            smem,
            pl.BlockSpec(f.shape, lambda i: (0, 0, 0, 0)),
            pl.BlockSpec((1, kn), lambda i: (0, 0)),
            pl.BlockSpec((kn, xb), lambda i: (0, i)),
            pl.BlockSpec((sb, 2, levels, wn), lambda i: (i, 0, 0, 0)),
            pl.BlockSpec((sb, 2, levels, wn), lambda i: (i, 0, 0, 0)),
            pl.BlockSpec((1, levels), lambda i: (0, 0)),
            pl.BlockSpec((1, wn), lambda i: (0, 0)),
        ],
        out_specs=(
            pl.BlockSpec((sb, 2, levels, wn), lambda i: (i, 0, 0, 0)),
            pl.BlockSpec((ln, rb, NLON), lambda i: (0, 0, 0)),
        ),
        scratch_shapes=[pltpu.VMEM((2 * ln * rb, kn), BF16)],
        compiler_params=pltpu.CompilerParams(vmem_limit_bytes=60_000_000),
        name="grid_rows",
    )(wave_of_slot, f, sign, t, spectral_state, forcing_noise, decay_row, amp_row)
    return (new_state, pattern)


def solution(mesh):
    return jax.shard_map(
        body,
        mesh=mesh,
        in_specs=(
            P("ma", None, None, "lev"),
            P("ma", None, None, "lev"),
            P(),
            P("lev"),
            P("ma", "lev", None),
            P(),
            P(),
        ),
        out_specs=(P("ma", None, None, "lev"), P("lev", "ma", None)),
        check_vma=False,
    )
```

```python
import math

import jax
import jax.numpy as jnp
from jax import lax
from jax.experimental import pallas as pl
from jax.experimental.pallas import tpu as pltpu
from jax.sharding import PartitionSpec as P

NLON = 2560
S = 16
H = S // 2
Q = S // 4
DEPTH = 4
RP = 128
BLOCKS = 5
MESH = pl.DeviceIdType.MESH
F32 = jnp.float32
BF16 = jnp.bfloat16


def cos_of(v):
    turns = jnp.round(v * F32(1.0 / NLON))
    y = (v - turns * F32(NLON)) * F32(2.0 * math.pi / NLON)
    y2 = y * y
    acc = jnp.full_like(y2, 1.0 / math.factorial(16))
    for k in range(7, -1, -1):
        acc = acc * y2 + F32((-1.0) ** k / math.factorial(2 * k))
    return acc


def column_of(row):
    n = row.shape[1]
    eye = lax.broadcasted_iota(jnp.int32, (n, n), 0) == lax.broadcasted_iota(jnp.int32, (n, n), 1)
    return jnp.sum(jnp.where(eye, jnp.broadcast_to(row, (n, n)), F32(0.0)), axis=1, keepdims=True)


def signed_rows(rows, sign, lhs):
    m = lhs.shape[0] // 2
    block = jnp.transpose(rows)[:m]
    flip = jnp.transpose(sign)
    flip = jnp.concatenate([flip] * (-(-m // RP)), axis=0)[:m]
    lhs[0:m, :] = block
    lhs[m:, :] = block * flip


def transform_kernel(
    wave_s, wave_v, lat_v, decay_v, amp_v, st_h, nz_h, lg_h,
    f_out, t_out, acc_out,
    stb, nzb, lgb, hv, pr, u1, ud, u2, d1, dd, d2, xf, xb, g, gb, fb, tb, mcol, latp, acc, lhs,
    ld_sem, swap_s, swap_r, ring_s, ring_r, a2a_s, a2a_r, out_sem,
):
    zn, ns, rows, jn = hv.shape
    ma_n = gb.shape[2]
    nc = ns // S
    last = nc - 1
    levels = stb.shape[4]
    wn = stb.shape[5]
    mn = wave_v.shape[0]
    rb = lat_v.shape[0] // ma_n
    ln = acc.shape[0] // (2 * rb)
    half = acc.shape[1]
    kc = fb.shape[1]
    me_ma = lax.axis_index("ma")
    me_lev = lax.axis_index("lev")
    z = me_lev // 2
    core = me_lev % 2
    partner = z * 2 + 1 - core
    zu = lax.rem(z + 1, zn)
    zd = lax.rem(z + zn - 1, zn)
    zo = lax.rem(z + 2, zn)
    up = zu * 2 + core
    down = zd * 2 + core

    def load(u):
        b = u % DEPTH
        return [
            pltpu.make_async_copy(lg_h.at[u // 2, :, u % 2], lgb.at[b], ld_sem.at[b, 2]),
            pltpu.make_async_copy(st_h.at[u // 2, :, u % 2], stb.at[b], ld_sem.at[b, 0]),
            pltpu.make_async_copy(nz_h.at[u // 2, :, u % 2], nzb.at[b], ld_sem.at[b, 1]),
        ]

    barrier = pltpu.get_barrier_semaphore()
    for lev in (partner, up, down):
        pl.semaphore_signal(barrier, inc=1, device_id={"lev": lev}, device_id_type=MESH)

    def greet(o, carry):
        peer = lax.rem(me_ma + o, ma_n)
        pl.semaphore_signal(barrier, inc=1, device_id={"ma": peer}, device_id_type=MESH)
        pl.semaphore_signal(
            barrier, inc=1, device_id={"ma": peer, "lev": partner}, device_id_type=MESH
        )
        return carry

    for u in range(DEPTH):
        for cp in load(u):
            cp.start()
    lax.fori_loop(1, ma_n, greet, 0)

    dec = jnp.broadcast_to(column_of(decay_v[...].reshape(1, levels)), (levels, wn))
    amp = amp_v[...].reshape(1, wn)
    n_at = me_lev * wn + lax.broadcasted_iota(jnp.int32, (1, 1, wn), 2)

    def compute(u):
        b = u % DEPTH

        def slot(i, carry):
            side = i // Q
            at_slot = (u // 2) * S + side * H + (u % 2) * Q + i % Q
            m = wave_s[me_ma * ns + at_slot]
            x = dec[None] * stb[b, side, i % Q] + amp[None] * nzb[b, side, i % Q].astype(F32)
            x = jnp.where(n_at >= m, x, F32(0.0)).reshape(2, zn, 8, wn)
            odd = (((n_at - m) & 1) == 1).reshape(1, 1, 1, wn)
            even_part = jnp.where(odd, F32(0.0), x)
            odd_part = jnp.where(odd, x, F32(0.0))
            left = jnp.concatenate([even_part, odd_part], axis=2).astype(BF16)
            left = left.reshape(2 * zn * 16, wn)
            out = jnp.dot(left, lgb[b, side, i % Q], preferred_element_type=F32).astype(BF16)
            for p in range(2):
                for t in range(zn):
                    at = (p * zn + t) * 16
                    hv[t, at_slot, p * 16 : (p + 1) * 16, :] = out[at : at + 16]
            return carry

        lax.fori_loop(0, H, slot, 0)

    def swap(u):
        first = (u % 2) * Q
        return pltpu.make_async_remote_copy(
            src_ref=hv.at[:, pl.ds((u // 2) * S + (1 - core) * H + first, Q)],
            dst_ref=pr.at[:, pl.ds((u // 2) * H + first, Q)],
            send_sem=swap_s.at[u],
            recv_sem=swap_r.at[u],
            device_id={"lev": partner},
            device_id_type=MESH,
        )

    def stage(u):
        for cp in load(u):
            cp.wait()
        compute(u)
        if u + DEPTH < 2 * nc:
            for cp in load(u + DEPTH):
                cp.start()
        if u == 0:
            pl.semaphore_wait(barrier, 3 + 2 * (ma_n - 1))
        swap(u).start()

    def hop(c, kind):
        box = (u1, ud, u2, d1, dd, d2)[kind]
        plane = (zo, zu, zu, zo, zd, zd)[kind]
        part = (0, 1, 0, 1, 0, 1)[kind]
        return pltpu.make_async_remote_copy(
            src_ref=pr.at[plane, pl.ds(c * H + part * Q, Q)],
            dst_ref=box.at[pl.ds(c * Q, Q)],
            send_sem=ring_s.at[c, kind],
            recv_sem=ring_r.at[c, kind],
            device_id={"lev": up if kind < 3 else down},
            device_id_type=MESH,
        )

    def merge(c, kind, more=None):
        plane = (zo, zu, zu, zo, zd, zd)[kind]
        part = (0, 1, 0, 1, 0, 1)[kind]

        def one(i, carry):
            at = c * H + part * Q + i
            own = c * S + core * H + part * Q + i
            total = hv[plane, own].astype(F32) + pr[plane, at].astype(F32)
            if more is not None:
                total = total + more[c * Q + i].astype(F32)
            pr[plane, at] = total.astype(BF16)
            return carry

        lax.fori_loop(0, Q, one, 0)
        hop(c, kind).start()

    def far(c):
        swap(2 * c).wait_recv()
        merge(c, 0)
        if c == 0:
            merge(c, 4)
            stage(2)
        swap(2 * c + 1).wait_recv()
        merge(c, 3)
        if c == 0:
            merge(c, 1)

    def near(c):
        merge(c, 1)
        merge(c, 4)

    def relay(c):
        hop(c, 0).wait_recv()
        merge(c, 2, u1)
        hop(c, 3).wait_recv()
        merge(c, 5, d1)

    place = pl.ds(pl.multiple_of((me_ma * 2 + core) * 16, 16), 16)

    def landing(c):
        return fb.at[c] if c < last else f_out

    def finish(c):
        for kind in (1, 2, 4, 5):
            hop(c, kind).wait_recv()
        for part, (r1, r2) in enumerate(((u2, dd), (d2, ud))):

            def one(i, carry):
                at = part * Q + i
                total = hv[z, c * S + core * H + at].astype(F32) + pr[z, c * H + at].astype(F32)
                total = total + (r1[c * Q + i].astype(F32) + r2[c * Q + i].astype(F32))
                for k in range(jn // 128):
                    at_row = pl.ds(pl.multiple_of(at * rows, rows), rows)
                    xf[k, at_row, :] = total[:, k * 128 : (k + 1) * 128]
                return carry

            lax.fori_loop(0, Q, one, 0)
        for level in range(8):
            for k in range(jn // 128):
                north = []
                south = []
                for p in range(2):
                    even = xf[k, pl.ds(p * 16 + level, H, stride=rows), :]
                    odd = xf[k, pl.ds(p * 16 + 8 + level, H, stride=rows), :]
                    north.append(even + odd)
                    south.append(even - odd)
                at_row = slice(level * 16, (level + 1) * 16)
                at = k * 128
                xb[at_row, at : at + 128] = jnp.concatenate(north, axis=0).astype(BF16)
                xb[at_row, jn + at : jn + at + 128] = jnp.concatenate(south, axis=0).astype(BF16)
        lanes = gb.shape[4]

        def pick(i, carry):
            m2 = lax.rem(me_ma // 2 + i, ma_n // 2)
            out = jnp.dot(xb[...], g[m2], preferred_element_type=F32)
            for k in range(2):
                peer = m2 * 2 + k
                for tc in range(2):
                    parts = [
                        out[(tc * ln + level) * 16 : (tc * ln + level + 1) * 16, k * RP : k * RP + rb]
                        for level in range(ln)
                    ]
                    if lanes > ln * rb:
                        parts.append(jnp.zeros((16, lanes - ln * rb), F32))
                    gb[c, tc, peer] = jnp.concatenate(parts, axis=1).astype(BF16)
            for k in range(2):
                peer = m2 * 2 + k
                for tc in range(2):

                    @pl.when(jnp.logical_or(peer != me_ma, tc != core))
                    def _():
                        pltpu.make_async_remote_copy(
                            src_ref=gb.at[c, tc, peer],
                            dst_ref=landing(c).at[place, :],
                            send_sem=a2a_s,
                            recv_sem=a2a_r.at[c],
                            device_id={"ma": peer, "lev": z * 2 + tc},
                            device_id_type=MESH,
                        ).start()

            return carry

        lax.fori_loop(0, ma_n // 2, pick, 0)
        if c < last:
            landing(c)[place, :] = gb[c, core, me_ma]
        else:
            pltpu.make_async_copy(gb.at[c, core, me_ma], f_out.at[place, :], out_sem.at[2]).start()

    def selection():
        step = 128
        for m2 in range(ma_n // 2):
            latp[m2] = jnp.full((1, 2 * RP), -1, jnp.int32)
            for k in range(2):
                src = (m2 * 2 + k) * rb
                latp[m2, :, k * RP : k * RP + rb] = lat_v[...].reshape(1, ma_n * rb)[:, src : src + rb]

        def one(m2, carry):
            lat = latp[m2]
            for r0 in range(0, 2 * jn, step):
                k = r0 + lax.broadcasted_iota(jnp.int32, (step, 2 * RP), 0)
                k = k if r0 < jn else 3 * jn - 1 - k
                g[m2, r0 : r0 + step, :] = jnp.where(lat == k, F32(1.0), F32(0.0)).astype(BF16)
            return carry

        lax.fori_loop(0, ma_n // 2, one, 0)

    per = 2 * ma_n

    def table(c):
        def one(i, carry):
            block = c * per + i
            first = (i // 2) * ns + c * S + (i % 2) * H
            m = jnp.broadcast_to(mcol[pl.ds(pl.multiple_of(first, 8), 8), 0:1], (8, RP))
            at = pl.ds(pl.multiple_of(block * 16, 16), 16)
            v = m * lax.broadcasted_iota(jnp.int32, (8, RP), 1).astype(F32)
            turn = m * F32(RP)
            quarter = F32(NLON // 4)
            w = jnp.where(m == F32(0.0), F32(1.0), F32(2.0))
            re, im = w * cos_of(v), w * cos_of(v + quarter)
            tre, tim = cos_of(turn), cos_of(turn + quarter)
            for k in range(half // RP):
                if k:
                    re, im = re * tre - im * tim, re * tim + im * tre
                tb[at, k * RP : (k + 1) * RP] = jnp.concatenate([re, im], axis=0).astype(BF16)
            flip = F32(1.0) - F32(2.0) * (m - F32(2.0) * jnp.floor(m * F32(0.5)))
            tb[at, half:] = jnp.concatenate([flip, flip], axis=0).astype(BF16)
            return carry

        lax.fori_loop(0, per, one, 0, unroll=2)

    def send_table():
        return pltpu.make_async_copy(tb.at[pl.ds(last * kc, kc)], t_out, out_sem.at[0])

    def send_acc():
        return pltpu.make_async_copy(acc, acc_out, out_sem.at[1])

    def along(c):
        whole = fb.at[c, pl.ds(0, kc - 16)]
        pltpu.make_async_copy(whole, whole, a2a_r.at[c]).wait()
        at_row = slice(c * kc, (c + 1) * kc)
        signed_rows(fb[c], tb[at_row, half:], lhs)
        width = half // BLOCKS
        for k in range(BLOCKS):
            at = slice(k * width, (k + 1) * width)
            part = jnp.dot(lhs[...], tb[at_row, at], preferred_element_type=F32)
            acc[:, at] = part if c == 0 else acc[:, at] + part

    stage(0)
    stage(1)
    far(0)
    stage(3)
    for u in range(4, min(6, 2 * nc)):
        stage(u)
    far(1)
    relay(0)
    near(1)
    for c in range(2, nc):
        for u in range(2 * c + 2, min(2 * c + 4, 2 * nc)):
            stage(u)
        if c == 2:
            mcol[...] = jnp.transpose(
                jnp.broadcast_to(wave_v[...].reshape(1, mn).astype(F32), (8, mn))
            )
            selection()
        if c >= 3:
            finish(c - 3)
            table(c - 3)
        if c >= 4:
            along(c - 4)
        far(c)
        relay(c - 1)
        near(c)
    table(last - 2)
    table(last - 1)
    table(last)
    send_table().start()
    finish(last - 2)
    along(last - 3)
    relay(last)
    finish(last - 1)
    along(last - 2)
    finish(last)
    along(last - 1)
    send_acc().start()

    for u in range(2 * nc):
        swap(u).wait_send()
    for c in range(nc):
        for kind in range(6):
            hop(c, kind).wait_send()
    send_table().wait()
    send_acc().wait()
    pltpu.make_async_copy(gb.at[last, core, me_ma], f_out.at[place, :], out_sem.at[2]).wait()
    flat = gb.reshape(nc * 2 * ma_n, 16, gb.shape[4]).at[pl.ds(0, nc * (2 * ma_n - 1))]
    pltpu.make_async_copy(flat, flat, a2a_s).wait()
    whole = f_out.at[pl.ds(0, kc - 16)]
    pltpu.make_async_copy(whole, whole, a2a_r.at[last]).wait()


def grid_kernel(wave_s, f, sign, t, acc, st, nz, decay_v, amp_v, new_state, out, lhs):
    step = pl.program_id(0)
    ln, rb, width = out.shape
    half = width // 2
    xb = t.shape[1]

    @pl.when(step == 0)
    def _():
        signed_rows(f[...], sign[...], lhs)

    levels = st.shape[2]
    wn = st.shape[3]
    dec = jnp.broadcast_to(column_of(decay_v[...].reshape(1, levels)), (levels, wn))
    amp = amp_v[...].reshape(1, wn)
    n_at = lax.axis_index("lev") * wn + lax.broadcasted_iota(jnp.int32, (1, 1, wn), 2)
    first = lax.axis_index("ma") * (st.shape[0] * pl.num_programs(0)) + step * st.shape[0]

    part = (acc[...] + jnp.dot(lhs[...], t[...], preferred_element_type=F32)).astype(BF16)
    for k in range(2):
        at = pl.ds(pl.multiple_of(k * half + step * xb, 128), xb)
        for level in range(ln):
            r0 = (k * ln + level) * rb
            out[level, :, at] = part[r0 : r0 + rb]
    for i in range(st.shape[0]):
        m = wave_s[first + i]
        x = dec[None] * st[i] + amp[None] * nz[i].astype(F32)
        new_state[i] = jnp.where(n_at >= m, x, F32(0.0))


def body(spectral_state, forcing_noise, decay_rate, amplitude, legendre, wave_of_slot, lat_of_row):
    ns, _, levels, wn = spectral_state.shape
    jn = legendre.shape[2]
    nlat = lat_of_row.shape[0]
    mn = wave_of_slot.shape[0]
    ma_n = mn // ns
    lev_n = lax.axis_size("lev")
    zn = lev_n // 2
    ln = levels // lev_n
    rb = nlat // ma_n
    nc = ns // S
    kn = 2 * mn
    kc = kn // nc
    half = NLON // 2
    lanes = -(-(ln * rb) // 128) * 128

    smem = pl.BlockSpec(memory_space=pltpu.SMEM)
    vmem = pl.BlockSpec(memory_space=pltpu.VMEM)
    hbm = pl.BlockSpec(memory_space=pl.ANY)
    box = pltpu.VMEM((nc * Q, 32, jn), BF16)
    dma = pltpu.SemaphoreType.DMA
    f, t, acc = pl.pallas_call(
        transform_kernel,
        out_shape=(
            jax.ShapeDtypeStruct((kc, lanes), BF16),
            jax.ShapeDtypeStruct((kc, half + RP), BF16),
            jax.ShapeDtypeStruct((2 * ln * rb, half), F32),
        ),
        in_specs=[smem, vmem, vmem, vmem, vmem, hbm, hbm, hbm],
        out_specs=(hbm, hbm, hbm),
        scratch_shapes=[
            pltpu.VMEM((DEPTH, 2, Q, 2, levels, wn), F32),
            pltpu.VMEM((DEPTH, 2, Q, 2, levels, wn), BF16),
            pltpu.VMEM((DEPTH, 2, Q, wn, jn), BF16),
            pltpu.VMEM((zn, ns, 32, jn), BF16),
            pltpu.VMEM((zn, ns // 2, 32, jn), BF16),
            box, box, box, box, box, box,
            pltpu.VMEM((jn // 128, H * 32, 128), F32),
            pltpu.VMEM((128, 2 * jn), BF16),
            pltpu.VMEM((ma_n // 2, 2 * jn, 2 * RP), BF16),
            pltpu.VMEM((nc, 2, ma_n, 16, lanes), BF16),
            pltpu.VMEM((nc - 1, kc, lanes), BF16),
            pltpu.VMEM((kn, half + RP), BF16),
            pltpu.VMEM((mn, 8), F32),
            pltpu.VMEM((ma_n // 2, 1, 2 * RP), jnp.int32),
            pltpu.VMEM((2 * ln * rb, half), F32),
            pltpu.VMEM((2 * ln * rb, kc), BF16),
            dma((DEPTH, 3)),
            dma((2 * nc,)),
            dma((2 * nc,)),
            dma((nc, 6)),
            dma((nc, 6)),
            dma,
            dma((nc,)),
            dma((3,)),
        ],
        compiler_params=pltpu.CompilerParams(
            collective_id=0, has_side_effects=True, vmem_limit_bytes=66_000_000
        ),
        name="transform",
    )(
        wave_of_slot, wave_of_slot, lat_of_row, decay_rate, amplitude,
        spectral_state.reshape(nc, 2, 2, Q, 2, levels, wn),
        forcing_noise.reshape(nc, 2, 2, Q, 2, levels, wn),
        legendre.reshape(nc, 2, 2, Q, wn, jn),
    )

    sb = ns // BLOCKS
    xb = half // BLOCKS
    new_state, pattern = pl.pallas_call(
        grid_kernel,
        grid=(BLOCKS,),
        out_shape=(
            jax.ShapeDtypeStruct((ns, 2, levels, wn), F32),
            jax.ShapeDtypeStruct((ln, rb, NLON), BF16),
        ),
        in_specs=[
            smem,
            pl.BlockSpec(f.shape, lambda i: (0, 0)),
            pl.BlockSpec((kc, RP), lambda i: (0, half // RP)),
            pl.BlockSpec((kc, xb), lambda i: (0, i)),
            pl.BlockSpec((2 * ln * rb, xb), lambda i: (0, i)),
            pl.BlockSpec((sb, 2, levels, wn), lambda i: (i, 0, 0, 0)),
            pl.BlockSpec((sb, 2, levels, wn), lambda i: (i, 0, 0, 0)),
            vmem,
            vmem,
        ],
        out_specs=(
            pl.BlockSpec((sb, 2, levels, wn), lambda i: (i, 0, 0, 0)),
            pl.BlockSpec((ln, rb, NLON), lambda i: (0, 0, 0)),
        ),
        scratch_shapes=[pltpu.VMEM((2 * ln * rb, kc), BF16)],
        compiler_params=pltpu.CompilerParams(vmem_limit_bytes=60_000_000),
        name="grid_rows",
    )(wave_of_slot, f, t, t, acc, spectral_state, forcing_noise, decay_rate, amplitude)
    return (new_state, pattern)


def solution(mesh):
    return jax.shard_map(
        body,
        mesh=mesh,
        in_specs=(
            P("ma", None, None, "lev"),
            P("ma", None, None, "lev"),
            P(),
            P("lev"),
            P("ma", "lev", None),
            P(),
            P(),
        ),
        out_specs=(P("ma", None, None, "lev"), P("lev", "ma", None)),
        check_vma=False,
    )
```

```python
import math

import jax
import jax.numpy as jnp
from jax import lax
from jax.experimental import pallas as pl
from jax.experimental.pallas import tpu as pltpu
from jax.sharding import PartitionSpec as P

NLON = 2560
S = 16
H = S // 2
Q = S // 4
DEPTH = 4
RP = 128
BLOCKS = 5
MESH = pl.DeviceIdType.MESH
F32 = jnp.float32
BF16 = jnp.bfloat16


def cos_of(v):
    turns = jnp.round(v * F32(1.0 / NLON))
    y = (v - turns * F32(NLON)) * F32(2.0 * math.pi / NLON)
    y2 = y * y
    acc = jnp.full_like(y2, 1.0 / math.factorial(16))
    for k in range(7, -1, -1):
        acc = acc * y2 + F32((-1.0) ** k / math.factorial(2 * k))
    return acc


def column_of(row):
    n = row.shape[1]
    eye = lax.broadcasted_iota(jnp.int32, (n, n), 0) == lax.broadcasted_iota(jnp.int32, (n, n), 1)
    return jnp.sum(jnp.where(eye, jnp.broadcast_to(row, (n, n)), F32(0.0)), axis=1, keepdims=True)


def signed_rows(rows, sign, lhs):
    m = lhs.shape[0] // 2
    block = jnp.transpose(rows)[:m]
    flip = jnp.transpose(sign)
    flip = jnp.concatenate([flip] * (-(-m // RP)), axis=0)[:m]
    lhs[0:m, :] = block
    lhs[m:, :] = block * flip


def transform_kernel(
    wave_h, lat_h, decay_h, amp_h, st_h, nz_h, lg_h,
    f_out, t_out, acc_out, ns_out,
    wave_s, wave_v, lat_v, decay_v, amp_v, stb, nzb, nsb, lgb, hv, pr, u1, ud, u2, d1, dd, d2, xf, xb, g, gb, fb, tb, mcol, latp, acc, accb, lhs,
    small_sem, ns_sem, ld_sem, swap_s, swap_r, ring_s, ring_r, a2a_s, a2a_r, out_sem,
):
    zn, ns, rows, jn = hv.shape
    ma_n = gb.shape[2]
    nc = ns // S
    last = nc - 1
    levels = stb.shape[4]
    wn = stb.shape[5]
    mn = wave_v.shape[0]
    rb = lat_v.shape[0] // ma_n
    ln = acc.shape[0] // (2 * rb)
    half = acc.shape[1]
    kc = fb.shape[1]
    me_ma = lax.axis_index("ma")
    me_lev = lax.axis_index("lev")
    z = me_lev // 2
    core = me_lev % 2
    partner = z * 2 + 1 - core
    zu = lax.rem(z + 1, zn)
    zd = lax.rem(z + zn - 1, zn)
    zo = lax.rem(z + 2, zn)
    up = zu * 2 + core
    down = zd * 2 + core

    def load(u, k):
        b = u % DEPTH
        side = (1 - core, core)[k]
        return [
            pltpu.make_async_copy(src.at[u // 2, side, u % 2], dst.at[b, k], ld_sem.at[b, k, n])
            for n, (src, dst) in enumerate(((lg_h, lgb), (st_h, stb), (nz_h, nzb)))
        ]

    def fetch(u):
        for cp in load(u, 0) + load(u, 1):
            cp.start()

    barrier = pltpu.get_barrier_semaphore()
    for lev in (partner, up, down):
        pl.semaphore_signal(barrier, inc=1, device_id={"lev": lev}, device_id_type=MESH)

    def greet(o, carry):
        peer = lax.rem(me_ma + o, ma_n)
        pl.semaphore_signal(barrier, inc=1, device_id={"ma": peer}, device_id_type=MESH)
        pl.semaphore_signal(
            barrier, inc=1, device_id={"ma": peer, "lev": partner}, device_id_type=MESH
        )
        return carry

    small = [
        pltpu.make_async_copy(src, dst, small_sem.at[k])
        for k, (src, dst) in enumerate(
            (
                (wave_h, wave_s),
                (decay_h, decay_v),
                (amp_h, amp_v),
                (wave_h, wave_v),
                (lat_h, lat_v),
            )
        )
    ]
    for cp in small[:3] + load(0, 0) + load(0, 1):
        cp.start()
    lax.fori_loop(1, ma_n, greet, 0)
    for cp in small[:3]:
        cp.wait()
    dec = jnp.broadcast_to(column_of(decay_v[...].reshape(1, levels)), (levels, wn))
    amp = amp_v[...].reshape(1, wn)
    n_at = me_lev * wn + lax.broadcasted_iota(jnp.int32, (1, 1, wn), 2)

    def compute(u, k):
        b = u % DEPTH
        side = (1 - core, core)[k]

        def slot(i, carry):
            at_slot = (u // 2) * S + side * H + (u % 2) * Q + i
            m = wave_s[me_ma * ns + at_slot]
            x = dec[None] * stb[b, k, i] + amp[None] * nzb[b, k, i].astype(F32)
            x = jnp.where(n_at >= m, x, F32(0.0))
            nsb[b, k, i] = x
            x = x.reshape(2, zn, 8, wn)
            odd = (((n_at - m) & 1) == 1).reshape(1, 1, 1, wn)
            even_part = jnp.where(odd, F32(0.0), x)
            odd_part = jnp.where(odd, x, F32(0.0))
            left = jnp.concatenate([even_part, odd_part], axis=2).astype(BF16)
            left = left.reshape(2 * zn * 16, wn)
            out = jnp.dot(left, lgb[b, k, i], preferred_element_type=F32).astype(BF16)
            for p in range(2):
                for t in range(zn):
                    at = (p * zn + t) * 16
                    hv[t, at_slot, p * 16 : (p + 1) * 16, :] = out[at : at + 16]
            return carry

        lax.fori_loop(0, Q, slot, 0, unroll=2)

    def swap(u):
        first = (u % 2) * Q
        return pltpu.make_async_remote_copy(
            src_ref=hv.at[:, pl.ds((u // 2) * S + (1 - core) * H + first, Q)],
            dst_ref=pr.at[:, pl.ds((u // 2) * H + first, Q)],
            send_sem=swap_s.at[u],
            recv_sem=swap_r.at[u],
            device_id={"lev": partner},
            device_id_type=MESH,
        )

    def keep(u):
        b = u % DEPTH
        return [
            pltpu.make_async_copy(
                nsb.at[b, k], ns_out.at[u // 2, (1 - core, core)[k], u % 2], ns_sem.at[b, k]
            )
            for k in range(2)
        ]

    def stage(u):
        for cp in load(u, 0):
            cp.wait()
        if u == 0:
            fetch(1)
        if u >= DEPTH:
            for cp in keep(u - DEPTH):
                cp.wait()
        compute(u, 0)
        if u == 0:
            pl.semaphore_wait(barrier, 3 + 2 * (ma_n - 1))
        swap(u).start()
        for cp in load(u, 1):
            cp.wait()
        if u == 0:
            for v in range(2, DEPTH):
                fetch(v)
            for cp in small[3:]:
                cp.start()
        compute(u, 1)
        for cp in keep(u):
            cp.start()
        if u + DEPTH < 2 * nc:
            fetch(u + DEPTH)

    def hop(c, kind):
        box = (u1, ud, u2, d1, dd, d2)[kind]
        plane = (zo, zu, zu, zo, zd, zd)[kind]
        part = (0, 1, 0, 1, 0, 1)[kind]
        return pltpu.make_async_remote_copy(
            src_ref=pr.at[plane, pl.ds(c * H + part * Q, Q)],
            dst_ref=box.at[pl.ds(c * Q, Q)],
            send_sem=ring_s.at[c, kind],
            recv_sem=ring_r.at[c, kind],
            device_id={"lev": up if kind < 3 else down},
            device_id_type=MESH,
        )

    def merge(c, kind, more=None):
        plane = (zo, zu, zu, zo, zd, zd)[kind]
        part = (0, 1, 0, 1, 0, 1)[kind]

        def one(i, carry):
            at = c * H + part * Q + i
            own = c * S + core * H + part * Q + i
            total = hv[plane, own].astype(F32) + pr[plane, at].astype(F32)
            if more is not None:
                total = total + more[c * Q + i].astype(F32)
            pr[plane, at] = total.astype(BF16)
            return carry

        lax.fori_loop(0, Q, one, 0)
        hop(c, kind).start()

    def far(c):
        swap(2 * c).wait_recv()
        merge(c, 0)
        if c == 0:
            merge(c, 4)
            stage(2)
        swap(2 * c + 1).wait_recv()
        merge(c, 3)
        if c == 0:
            merge(c, 1)

    def near(c):
        merge(c, 1)
        merge(c, 4)

    def relay(c):
        hop(c, 0).wait_recv()
        merge(c, 2, u1)
        hop(c, 3).wait_recv()
        merge(c, 5, d1)

    place = pl.ds(pl.multiple_of((me_ma * 2 + core) * 16, 16), 16)

    def landing(c):
        return fb.at[c] if c < last else f_out

    def finish(c):
        for kind in (1, 2, 4, 5):
            hop(c, kind).wait_recv()
        for part, (r1, r2) in enumerate(((u2, dd), (d2, ud))):

            def one(i, carry):
                at = part * Q + i
                total = hv[z, c * S + core * H + at].astype(F32) + pr[z, c * H + at].astype(F32)
                total = total + (r1[c * Q + i].astype(F32) + r2[c * Q + i].astype(F32))
                for k in range(jn // 128):
                    at_row = pl.ds(pl.multiple_of(at * rows, rows), rows)
                    xf[k, at_row, :] = total[:, k * 128 : (k + 1) * 128]
                return carry

            lax.fori_loop(0, Q, one, 0)
        for level in range(8):
            for k in range(jn // 128):
                north = []
                south = []
                for p in range(2):
                    even = xf[k, pl.ds(p * 16 + level, H, stride=rows), :]
                    odd = xf[k, pl.ds(p * 16 + 8 + level, H, stride=rows), :]
                    north.append(even + odd)
                    south.append(even - odd)
                at_row = slice(level * 16, (level + 1) * 16)
                at = k * 128
                xb[at_row, at : at + 128] = jnp.concatenate(north, axis=0).astype(BF16)
                xb[at_row, jn + at : jn + at + 128] = jnp.concatenate(south, axis=0).astype(BF16)
        lanes = gb.shape[4]

        def pick(i, carry):
            pairs = ma_n // 2
            m2 = lax.rem(me_ma // 2 + pairs + pairs // 2 + (2 * (i % 2) - 1) * ((i + 1) // 2), pairs)
            out = jnp.dot(xb[...], g[m2], preferred_element_type=F32)
            for k in range(2):
                peer = m2 * 2 + k
                for tc in range(2):
                    parts = [
                        out[(tc * ln + level) * 16 : (tc * ln + level + 1) * 16, k * RP : k * RP + rb]
                        for level in range(ln)
                    ]
                    if lanes > ln * rb:
                        parts.append(jnp.zeros((16, lanes - ln * rb), F32))
                    gb[c, tc, peer] = jnp.concatenate(parts, axis=1).astype(BF16)
            for k in range(2):
                peer = m2 * 2 + k
                for tc in range(2):

                    @pl.when(jnp.logical_or(peer != me_ma, tc != core))
                    def _():
                        pltpu.make_async_remote_copy(
                            src_ref=gb.at[c, tc, peer],
                            dst_ref=landing(c).at[place, :],
                            send_sem=a2a_s,
                            recv_sem=a2a_r.at[c],
                            device_id={"ma": peer, "lev": z * 2 + tc},
                            device_id_type=MESH,
                        ).start()

            return carry

        lax.fori_loop(0, ma_n // 2, pick, 0)
        if c < last:
            landing(c)[place, :] = gb[c, core, me_ma]
        else:
            pltpu.make_async_copy(gb.at[c, core, me_ma], f_out.at[place, :], out_sem.at[2]).start()

    def selection():
        step = 128
        for m2 in range(ma_n // 2):
            latp[m2] = jnp.full((1, 2 * RP), -1, jnp.int32)
            for k in range(2):
                src = (m2 * 2 + k) * rb
                latp[m2, :, k * RP : k * RP + rb] = lat_v[...].reshape(1, ma_n * rb)[:, src : src + rb]

        def one(m2, carry):
            lat = latp[m2]
            for r0 in range(0, 2 * jn, step):
                k = r0 + lax.broadcasted_iota(jnp.int32, (step, 2 * RP), 0)
                k = k if r0 < jn else 3 * jn - 1 - k
                g[m2, r0 : r0 + step, :] = jnp.where(lat == k, F32(1.0), F32(0.0)).astype(BF16)
            return carry

        lax.fori_loop(0, ma_n // 2, one, 0)

    per = 2 * ma_n

    def table(c):
        def one(i, carry):
            block = c * per + i
            first = (i // 2) * ns + c * S + (i % 2) * H
            m = jnp.broadcast_to(mcol[pl.ds(pl.multiple_of(first, 8), 8), 0:1], (8, RP))
            at = pl.ds(pl.multiple_of(block * 16, 16), 16)
            v = m * lax.broadcasted_iota(jnp.int32, (8, RP), 1).astype(F32)
            turn = m * F32(RP)
            quarter = F32(NLON // 4)
            w = jnp.where(m == F32(0.0), F32(1.0), F32(2.0))
            re, im = w * cos_of(v), w * cos_of(v + quarter)
            tre, tim = cos_of(turn), cos_of(turn + quarter)
            for k in range(half // RP):
                if k:
                    re, im = re * tre - im * tim, re * tim + im * tre
                tb[at, k * RP : (k + 1) * RP] = jnp.concatenate([re, im], axis=0).astype(BF16)
            flip = F32(1.0) - F32(2.0) * (m - F32(2.0) * jnp.floor(m * F32(0.5)))
            tb[at, half:] = jnp.concatenate([flip, flip], axis=0).astype(BF16)
            return carry

        lax.fori_loop(0, per, one, 0, unroll=2)

    def send_table():
        return pltpu.make_async_copy(tb.at[pl.ds(last * kc, kc)], t_out, out_sem.at[0])

    def send_acc():
        return pltpu.make_async_copy(accb, acc_out, out_sem.at[1])

    def along(c):
        whole = fb.at[c, pl.ds(0, kc - 16)]
        pltpu.make_async_copy(whole, whole, a2a_r.at[c]).wait()
        at_row = slice(c * kc, (c + 1) * kc)
        signed_rows(fb[c], tb[at_row, half:], lhs)
        width = half // BLOCKS
        for k in range(BLOCKS):
            at = slice(k * width, (k + 1) * width)
            part = jnp.dot(lhs[...], tb[at_row, at], preferred_element_type=F32)
            total = part if c == 0 else acc[:, at] + part
            if c < last - 1:
                acc[:, at] = total
            else:
                accb[:, at] = total.astype(BF16)

    stage(0)
    stage(1)
    far(0)
    stage(3)
    far(1)
    stage(4)
    relay(0)
    near(1)
    for c in range(2, nc):
        stage(2 * c + 1)
        if c == 2:
            for cp in small[3:]:
                cp.wait()
            mcol[...] = jnp.transpose(
                jnp.broadcast_to(wave_v[...].reshape(1, mn).astype(F32), (8, mn))
            )
            selection()
        if c >= 3:
            finish(c - 3)
            table(c - 3)
        if c >= 4:
            along(c - 4)
        far(c)
        if c < last:
            stage(2 * c + 2)
        relay(c - 1)
        near(c)
    table(last - 2)
    table(last - 1)
    table(last)
    send_table().start()
    finish(last - 2)
    along(last - 3)
    relay(last)
    finish(last - 1)
    along(last - 2)
    finish(last)
    along(last - 1)
    send_acc().start()

    for u in range(2 * nc):
        swap(u).wait_send()
    for u in range(2 * nc - DEPTH, 2 * nc):
        for cp in keep(u):
            cp.wait()
    for c in range(nc):
        for kind in range(6):
            hop(c, kind).wait_send()
    send_table().wait()
    send_acc().wait()
    pltpu.make_async_copy(gb.at[last, core, me_ma], f_out.at[place, :], out_sem.at[2]).wait()
    flat = gb.reshape(nc * 2 * ma_n, 16, gb.shape[4]).at[pl.ds(0, nc * (2 * ma_n - 1))]
    pltpu.make_async_copy(flat, flat, a2a_s).wait()
    whole = f_out.at[pl.ds(0, kc - 16)]
    pltpu.make_async_copy(whole, whole, a2a_r.at[last]).wait()


def grid_kernel(f_h, t_h, acc_h, kept_h, new_h, out_h, f, t, acc, kept, lhs, obuf, in_sem, keep_sem, out_sem):
    ln, rb, width = out_h.shape
    half = width // 2
    xb = half // BLOCKS
    parts = kept_h.shape[0]

    first = [
        pltpu.make_async_copy(f_h, f, in_sem.at[0]),
        pltpu.make_async_copy(t_h, t, in_sem.at[1]),
        pltpu.make_async_copy(acc_h, acc, in_sem.at[2]),
    ]
    take = [
        pltpu.make_async_copy(kept_h.at[c], kept.at[c], keep_sem.at[0, c]) for c in range(parts)
    ]
    give = [
        pltpu.make_async_copy(kept.at[c], new_h.at[c], keep_sem.at[1, c]) for c in range(parts)
    ]

    def store(k):
        return [
            pltpu.make_async_copy(
                obuf.at[k, p],
                out_h.at[:, :, pl.ds(p * half + k * xb, xb)],
                out_sem.at[k, p],
            )
            for p in range(2)
        ]

    for cp in first[:2] + take[:2] + first[2:] + take[2:]:
        cp.start()
    first[0].wait()
    first[1].wait()
    signed_rows(f[...], t[:, half:], lhs)
    first[2].wait()
    for k in range(max(BLOCKS, parts)):
        if k < parts:
            take[k].wait()
            give[k].start()
        if k < BLOCKS:
            at = slice(k * xb, (k + 1) * xb)
            part = jnp.dot(lhs[...], t[:, at], preferred_element_type=F32)
            part = (acc[:, at].astype(F32) + part).astype(BF16)
            for p in range(2):
                for level in range(ln):
                    r0 = (p * ln + level) * rb
                    obuf[k, p, level] = part[r0 : r0 + rb]
            for cp in store(k):
                cp.start()
    for k in range(BLOCKS):
        for cp in store(k):
            cp.wait()
    for cp in give:
        cp.wait()


def body(spectral_state, forcing_noise, decay_rate, amplitude, legendre, wave_of_slot, lat_of_row):
    ns, _, levels, wn = spectral_state.shape
    jn = legendre.shape[2]
    nlat = lat_of_row.shape[0]
    mn = wave_of_slot.shape[0]
    ma_n = mn // ns
    lev_n = lax.axis_size("lev")
    zn = lev_n // 2
    ln = levels // lev_n
    rb = nlat // ma_n
    nc = ns // S
    kn = 2 * mn
    kc = kn // nc
    half = NLON // 2
    lanes = -(-(ln * rb) // 128) * 128

    smem = pl.BlockSpec(memory_space=pltpu.SMEM)
    vmem = pl.BlockSpec(memory_space=pltpu.VMEM)
    hbm = pl.BlockSpec(memory_space=pl.ANY)
    box = pltpu.VMEM((nc * Q, 32, jn), BF16)
    dma = pltpu.SemaphoreType.DMA
    f, t, acc, kept = pl.pallas_call(
        transform_kernel,
        out_shape=(
            jax.ShapeDtypeStruct((kc, lanes), BF16),
            jax.ShapeDtypeStruct((kc, half + RP), BF16),
            jax.ShapeDtypeStruct((2 * ln * rb, half), BF16),
            jax.ShapeDtypeStruct((nc, 2, 2, Q, 2, levels, wn), F32),
        ),
        in_specs=[hbm] * 7,
        out_specs=(hbm,) * 4,
        scratch_shapes=[
            pltpu.SMEM((mn,), jnp.int32),
            pltpu.VMEM((mn,), jnp.int32),
            pltpu.VMEM((nlat,), jnp.int32),
            pltpu.VMEM((levels,), F32),
            pltpu.VMEM((wn,), F32),
            pltpu.VMEM((DEPTH, 2, Q, 2, levels, wn), F32),
            pltpu.VMEM((DEPTH, 2, Q, 2, levels, wn), BF16),
            pltpu.VMEM((DEPTH, 2, Q, 2, levels, wn), F32),
            pltpu.VMEM((DEPTH, 2, Q, wn, jn), BF16),
            pltpu.VMEM((zn, ns, 32, jn), BF16),
            pltpu.VMEM((zn, ns // 2, 32, jn), BF16),
            box, box, box, box, box, box,
            pltpu.VMEM((jn // 128, H * 32, 128), F32),
            pltpu.VMEM((128, 2 * jn), BF16),
            pltpu.VMEM((ma_n // 2, 2 * jn, 2 * RP), BF16),
            pltpu.VMEM((nc, 2, ma_n, 16, lanes), BF16),
            pltpu.VMEM((nc - 1, kc, lanes), BF16),
            pltpu.VMEM((kn, half + RP), BF16),
            pltpu.VMEM((mn, 8), F32),
            pltpu.VMEM((ma_n // 2, 1, 2 * RP), jnp.int32),
            pltpu.VMEM((2 * ln * rb, half), F32),
            pltpu.VMEM((2 * ln * rb, half), BF16),
            pltpu.VMEM((2 * ln * rb, kc), BF16),
            dma((5,)),
            dma((DEPTH, 2)),
            dma((DEPTH, 2, 3)),
            dma((2 * nc,)),
            dma((2 * nc,)),
            dma((nc, 6)),
            dma((nc, 6)),
            dma,
            dma((nc,)),
            dma((3,)),
        ],
        compiler_params=pltpu.CompilerParams(
            collective_id=0, has_side_effects=True, vmem_limit_bytes=66_000_000
        ),
        name="transform",
    )(
        wave_of_slot, lat_of_row, decay_rate, amplitude,
        spectral_state.reshape(nc, 2, 2, Q, 2, levels, wn),
        forcing_noise.reshape(nc, 2, 2, Q, 2, levels, wn),
        legendre.reshape(nc, 2, 2, Q, wn, jn),
    )

    xb = half // BLOCKS
    new_state, pattern = pl.pallas_call(
        grid_kernel,
        out_shape=(
            jax.ShapeDtypeStruct((nc, S, 2, levels, wn), F32),
            jax.ShapeDtypeStruct((ln, rb, NLON), BF16),
        ),
        in_specs=[hbm] * 4,
        out_specs=(hbm, hbm),
        scratch_shapes=[
            pltpu.VMEM((kc, lanes), BF16),
            pltpu.VMEM((kc, half + RP), BF16),
            pltpu.VMEM((2 * ln * rb, half), BF16),
            pltpu.VMEM((nc, S, 2, levels, wn), F32),
            pltpu.VMEM((2 * ln * rb, kc), BF16),
            pltpu.VMEM((BLOCKS, 2, ln, rb, xb), BF16),
            dma((3,)),
            dma((2, nc)),
            dma((BLOCKS, 2)),
        ],
        compiler_params=pltpu.CompilerParams(vmem_limit_bytes=60_000_000),
        name="grid_rows",
    )(f, t, acc, kept.reshape(nc, S, 2, levels, wn))
    return (new_state.reshape(ns, 2, levels, wn), pattern)


def solution(mesh):
    return jax.shard_map(
        body,
        mesh=mesh,
        in_specs=(
            P("ma", None, None, "lev"),
            P("ma", None, None, "lev"),
            P(),
            P("lev"),
            P("ma", "lev", None),
            P(),
            P(),
        ),
        out_specs=(P("ma", None, None, "lev"), P("lev", "ma", None)),
        check_vma=False,
    )
```

```python
import math

import jax
import jax.numpy as jnp
from jax import lax
from jax.experimental import pallas as pl
from jax.experimental.pallas import tpu as pltpu
from jax.sharding import PartitionSpec as P

NLON = 2560
S = 16
H = S // 2
Q = S // 4
DEPTH = 3
ORDER = (0, 1, 2, 3, 8, 4, 5, 9, 6, 7)
RP = 128
BLOCKS = 5
MESH = pl.DeviceIdType.MESH
F32 = jnp.float32
BF16 = jnp.bfloat16


def cos_of(v):
    turns = jnp.round(v * F32(1.0 / NLON))
    y = (v - turns * F32(NLON)) * F32(2.0 * math.pi / NLON)
    y2 = y * y
    acc = jnp.full_like(y2, 1.0 / math.factorial(16))
    for k in range(7, -1, -1):
        acc = acc * y2 + F32((-1.0) ** k / math.factorial(2 * k))
    return acc


def column_of(row):
    n = row.shape[1]
    eye = lax.broadcasted_iota(jnp.int32, (n, n), 0) == lax.broadcasted_iota(jnp.int32, (n, n), 1)
    return jnp.sum(jnp.where(eye, jnp.broadcast_to(row, (n, n)), F32(0.0)), axis=1, keepdims=True)


def signed_rows(rows, sign, lhs):
    m = lhs.shape[0] // 2
    block = jnp.transpose(rows)[:m]
    flip = jnp.transpose(sign)
    flip = jnp.concatenate([flip] * (-(-m // RP)), axis=0)[:m]
    lhs[0:m, :] = block
    lhs[m:, :] = block * flip


def transform_kernel(
    wave_h, lat_h, decay_h, amp_h, st_h, nz_h, lg_h,
    f_out, t_out, acc_out, ns_out,
    wave_s, wave_v, lat_v, decay_v, amp_v, stb, nzb, nsb, lgb, hv, pr, u1, ud, u2, d1, dd, d2, perm, xn, xb, g, gb, gbs, fb, sa, sbox, tb, mcol, latp, acc, accb, lhs,
    small_sem, ns_sem, ld_sem, swap_s, swap_r, ring_s, ring_r, a2a_s, a2a_s2, a2a_r, out_sem,
):
    zn, ns, rows, jn = hv.shape
    ma_n = gb.shape[2]
    nc = ns // S
    assert 2 * nc == len(ORDER)
    last = nc - 1
    levels = stb.shape[4]
    wn = stb.shape[5]
    mn = wave_v.shape[0]
    rb = lat_v.shape[0] // ma_n
    ln = acc.shape[0] // (2 * rb)
    half = acc.shape[1]
    kc = fb.shape[1]
    me_ma = lax.axis_index("ma")
    me_lev = lax.axis_index("lev")
    z = me_lev // 2
    core = me_lev % 2
    partner = z * 2 + 1 - core
    zu = lax.rem(z + 1, zn)
    zd = lax.rem(z + zn - 1, zn)
    zo = lax.rem(z + 2, zn)
    up = zu * 2 + core
    down = zd * 2 + core

    def load(u, k):
        b = ORDER.index(u) % DEPTH
        side = (1 - core, core)[k]
        return [
            pltpu.make_async_copy(src.at[u // 2, side, u % 2], dst.at[b, k], ld_sem.at[b, k, n])
            for n, (src, dst) in enumerate(((lg_h, lgb), (st_h, stb), (nz_h, nzb)))
        ]

    def fetch(u):
        for cp in load(u, 0) + load(u, 1):
            cp.start()

    barrier = pltpu.get_barrier_semaphore()
    for lev in (partner, up, down):
        pl.semaphore_signal(barrier, inc=1, device_id={"lev": lev}, device_id_type=MESH)

    def greet(o, carry):
        peer = lax.rem(me_ma + o, ma_n)
        pl.semaphore_signal(barrier, inc=1, device_id={"ma": peer}, device_id_type=MESH)
        pl.semaphore_signal(
            barrier, inc=1, device_id={"ma": peer, "lev": partner}, device_id_type=MESH
        )
        return carry

    small = [
        pltpu.make_async_copy(src, dst, small_sem.at[k])
        for k, (src, dst) in enumerate(
            (
                (wave_h, wave_s),
                (decay_h, decay_v),
                (amp_h, amp_v),
                (wave_h, wave_v),
                (lat_h, lat_v),
            )
        )
    ]
    for cp in small[:3] + load(0, 0) + load(0, 1):
        cp.start()
    lax.fori_loop(1, ma_n, greet, 0)
    for cp in small[:3]:
        cp.wait()
    dec = jnp.broadcast_to(column_of(decay_v[...].reshape(1, levels)), (levels, wn))
    amp = amp_v[...].reshape(1, wn)
    n_at = me_lev * wn + lax.broadcasted_iota(jnp.int32, (1, 1, wn), 2)

    def compute(u, k):
        b = ORDER.index(u) % DEPTH
        side = (1 - core, core)[k]

        def slot(i, carry):
            at_slot = (u // 2) * S + side * H + (u % 2) * Q + i
            m = wave_s[me_ma * ns + at_slot]
            x = dec[None] * stb[b, k, i] + amp[None] * nzb[b, k, i].astype(F32)
            x = jnp.where(n_at >= m, x, F32(0.0))
            nsb[b, k, i] = x
            x = x.reshape(2, zn, 8, wn)
            odd = (((n_at - m) & 1) == 1).reshape(1, 1, 1, wn)
            even_part = jnp.where(odd, F32(0.0), x)
            odd_part = jnp.where(odd, x, F32(0.0))
            left = jnp.concatenate([even_part, odd_part], axis=2).astype(BF16)
            left = left.reshape(2 * zn * 16, wn)
            out = jnp.dot(left, lgb[b, k, i], preferred_element_type=F32).astype(BF16)
            for p in range(2):
                for t in range(zn):
                    at = (p * zn + t) * 16
                    hv[t, at_slot, p * 16 : (p + 1) * 16, :] = out[at : at + 16]
            return carry

        lax.fori_loop(0, Q, slot, 0, unroll=2)

    def swap(u):
        first = (u % 2) * Q
        return pltpu.make_async_remote_copy(
            src_ref=hv.at[:, pl.ds((u // 2) * S + (1 - core) * H + first, Q)],
            dst_ref=pr.at[:, pl.ds((u // 2) * H + first, Q)],
            send_sem=swap_s.at[u],
            recv_sem=swap_r.at[u],
            device_id={"lev": partner},
            device_id_type=MESH,
        )

    def keep(u):
        b = ORDER.index(u) % DEPTH
        return [
            pltpu.make_async_copy(
                nsb.at[b, k], ns_out.at[u // 2, (1 - core, core)[k], u % 2], ns_sem.at[b, k]
            )
            for k in range(2)
        ]

    def stage(u):
        for cp in load(u, 0):
            cp.wait()
        if u == 0:
            fetch(1)
        at = ORDER.index(u)
        if at >= DEPTH:
            for cp in keep(ORDER[at - DEPTH]):
                cp.wait()
        compute(u, 0)
        if u == 0:
            pl.semaphore_wait(barrier, 3 + 2 * (ma_n - 1))
        swap(u).start()
        for cp in load(u, 1):
            cp.wait()
        if u == 0:
            for v in ORDER[2:DEPTH]:
                fetch(v)
            for cp in small[3:]:
                cp.start()
        compute(u, 1)
        for cp in keep(u):
            cp.start()
        if at + DEPTH < 2 * nc:
            fetch(ORDER[at + DEPTH])

    def hop(c, kind):
        box = (u1, ud, u2, d1, dd, d2)[kind]
        plane = (zo, zu, zu, zo, zd, zd)[kind]
        part = (0, 1, 0, 1, 0, 1)[kind]
        return pltpu.make_async_remote_copy(
            src_ref=pr.at[plane, pl.ds(c * H + part * Q, Q)],
            dst_ref=box.at[pl.ds(c * Q, Q)],
            send_sem=ring_s.at[c, kind],
            recv_sem=ring_r.at[c, kind],
            device_id={"lev": up if kind < 3 else down},
            device_id_type=MESH,
        )

    def merge(c, kind, more=None):
        plane = (zo, zu, zu, zo, zd, zd)[kind]
        part = (0, 1, 0, 1, 0, 1)[kind]

        def one(i, carry):
            at = c * H + part * Q + i
            own = c * S + core * H + part * Q + i
            total = hv[plane, own].astype(F32) + pr[plane, at].astype(F32)
            if more is not None:
                total = total + more[c * Q + i].astype(F32)
            pr[plane, at] = total.astype(BF16)
            return carry

        lax.fori_loop(0, Q, one, 0)
        hop(c, kind).start()

    def far(c):
        swap(2 * c).wait_recv()
        merge(c, 0)
        if c == 0:
            merge(c, 4)
            stage(2)
        swap(2 * c + 1).wait_recv()
        merge(c, 3)
        if c == 0:
            merge(c, 1)

    def near(c):
        merge(c, 1)
        merge(c, 4)

    def relay(c):
        hop(c, 0).wait_recv()
        merge(c, 2, u1)
        hop(c, 3).wait_recv()
        merge(c, 5, d1)

    place = pl.ds(pl.multiple_of((me_ma * 2 + core) * 16, 16), 16)

    def fill(s, total):
        even = jnp.concatenate([total[0:8], total[16:24]], axis=0)
        odd = jnp.concatenate([total[8:16], total[24:32]], axis=0)
        at = pl.ds(pl.multiple_of(s * 16, 16), 16)
        xn[at, 0:jn] = (even + odd).astype(BF16)
        xn[at, jn:] = (even - odd).astype(BF16)

    def spread(box, land, recv_sem, send_sem):
        for k in range(2 * jn // 256):
            at = slice(k * 256, (k + 1) * 256)
            xb[:, at] = jnp.dot(perm[...], xn[:, at], preferred_element_type=F32).astype(BF16)
        lanes = box.shape[3]

        def pick(i, carry):
            pairs = ma_n // 2
            m2 = lax.rem(me_ma // 2 + pairs + pairs // 2 + (2 * (i % 2) - 1) * ((i + 1) // 2), pairs)
            out = jnp.dot(xb[...], g[m2], preferred_element_type=F32)
            for k in range(2):
                peer = m2 * 2 + k
                for tc in range(2):
                    parts = [
                        out[(tc * ln + level) * 16 : (tc * ln + level + 1) * 16, k * RP : k * RP + rb]
                        for level in range(ln)
                    ]
                    if lanes > ln * rb:
                        parts.append(jnp.zeros((16, lanes - ln * rb), F32))
                    box[tc, peer] = jnp.concatenate(parts, axis=1).astype(BF16)
            for k in range(2):
                peer = m2 * 2 + k
                for tc in range(2):

                    @pl.when(jnp.logical_or(peer != me_ma, tc != core))
                    def _():
                        pltpu.make_async_remote_copy(
                            src_ref=box.at[tc, peer],
                            dst_ref=land.at[place, :],
                            send_sem=send_sem,
                            recv_sem=recv_sem,
                            device_id={"ma": peer, "lev": z * 2 + tc},
                            device_id_type=MESH,
                        ).start()

            return carry

        lax.fori_loop(0, ma_n // 2, pick, 0, unroll=2 if ma_n > 2 else 1)
        land[place, :] = box[core, me_ma]

    def finish(c):
        for kind in (1, 2, 4, 5):
            hop(c, kind).wait_recv()
        for part, (r1, r2) in enumerate(((u2, dd), (d2, ud))):

            def one(i, carry):
                at = part * Q + i
                total = hv[z, c * S + core * H + at].astype(F32) + pr[z, c * H + at].astype(F32)
                fill(at, total + (r1[c * Q + i].astype(F32) + r2[c * Q + i].astype(F32)))
                return carry

            lax.fori_loop(0, Q, one, 0)
        spread(gb.at[c], fb.at[c], a2a_r.at[c], a2a_s)

    hk = kc // 2

    def early(k):
        plane = (zo, zu, zd, z)[k]

        def one(i, carry):
            total = hv[plane, last * S + core * H + i].astype(F32)
            fill(i, total + pr[plane, last * H + i].astype(F32))
            return carry

        lax.fori_loop(0, H, one, 0)
        spread(gbs.at[k], sa.at[k], a2a_r.at[last + k], a2a_s2)

    def arrived(k):
        whole = sa.at[k, pl.ds(0, kc - 16)]
        pltpu.make_async_copy(whole, whole, a2a_r.at[last + k]).wait()

    def late_hop(kind):
        k = (0, 1, 1, 0, 2, 2)[kind]
        part = (0, 1, 0, 1, 0, 1)[kind]
        return pltpu.make_async_remote_copy(
            src_ref=sa.at[k, pl.ds(part * hk, hk)],
            dst_ref=sbox.at[kind],
            send_sem=ring_s.at[last, kind],
            recv_sem=ring_r.at[last, kind],
            device_id={"lev": up if kind < 3 else down},
            device_id_type=MESH,
        )

    def add_rows(k, part, *kinds):
        def one(i, carry):
            at = pl.ds(pl.multiple_of(part * hk + i * 32, 32), 32)
            other = pl.ds(pl.multiple_of(i * 32, 32), 32)
            total = sa[k, at, :].astype(F32)
            for kind in kinds:
                total = total + sbox[kind, other, :].astype(F32)
            sa[k, at, :] = total.astype(BF16)
            return carry

        lax.fori_loop(0, hk // 32, one, 0)

    def late_far():
        arrived(0)
        late_hop(0).start()
        late_hop(3).start()

    def late_near():
        arrived(1)
        late_hop(1).start()
        arrived(2)
        late_hop(4).start()

    def late_relay():
        late_hop(0).wait_recv()
        add_rows(1, 0, 0)
        late_hop(2).start()
        late_hop(3).wait_recv()
        add_rows(2, 1, 3)
        late_hop(5).start()

    def send_rows():
        return pltpu.make_async_copy(sa.at[3], f_out, out_sem.at[2])

    def late_finish():
        arrived(3)
        for kind in (1, 2, 4, 5):
            late_hop(kind).wait_recv()
        add_rows(3, 0, 2, 4)
        add_rows(3, 1, 5, 1)
        send_rows().start()

    def selection():
        step = 128
        to = lax.broadcasted_iota(jnp.int32, (128, 128), 0)
        came = lax.broadcasted_iota(jnp.int32, (128, 128), 1)
        to = (to % 8) * 16 + (to // 8 % 2) * 8 + to // 16
        perm[...] = jnp.where(to == came, F32(1.0), F32(0.0)).astype(BF16)
        for m2 in range(ma_n // 2):
            latp[m2] = jnp.full((1, 2 * RP), -1, jnp.int32)
            for k in range(2):
                src = (m2 * 2 + k) * rb
                latp[m2, :, k * RP : k * RP + rb] = lat_v[...].reshape(1, ma_n * rb)[:, src : src + rb]

        def one(m2, carry):
            lat = latp[m2]
            for r0 in range(0, 2 * jn, step):
                k = r0 + lax.broadcasted_iota(jnp.int32, (step, 2 * RP), 0)
                k = k if r0 < jn else 3 * jn - 1 - k
                g[m2, r0 : r0 + step, :] = jnp.where(lat == k, F32(1.0), F32(0.0)).astype(BF16)
            return carry

        lax.fori_loop(0, ma_n // 2, one, 0)

    per = 2 * ma_n

    def table(c):
        def one(i, carry):
            block = c * per + i
            first = (i // 2) * ns + c * S + (i % 2) * H
            m = jnp.broadcast_to(mcol[pl.ds(pl.multiple_of(first, 8), 8), 0:1], (8, RP))
            at = pl.ds(pl.multiple_of(block * 16, 16), 16)
            v = m * lax.broadcasted_iota(jnp.int32, (8, RP), 1).astype(F32)
            turn = m * F32(RP)
            quarter = F32(NLON // 4)
            w = jnp.where(m == F32(0.0), F32(1.0), F32(2.0))
            re, im = w * cos_of(v), w * cos_of(v + quarter)
            tre, tim = cos_of(turn), cos_of(turn + quarter)
            for k in range(half // RP):
                if k:
                    re, im = re * tre - im * tim, re * tim + im * tre
                tb[at, k * RP : (k + 1) * RP] = jnp.concatenate([re, im], axis=0).astype(BF16)
            flip = F32(1.0) - F32(2.0) * (m - F32(2.0) * jnp.floor(m * F32(0.5)))
            tb[at, half:] = jnp.concatenate([flip, flip], axis=0).astype(BF16)
            return carry

        lax.fori_loop(0, per, one, 0, unroll=8 if per % 8 == 0 else 4)

    def send_table():
        return pltpu.make_async_copy(tb.at[pl.ds(last * kc, kc)], t_out, out_sem.at[0])

    def send_acc():
        return pltpu.make_async_copy(accb, acc_out, out_sem.at[1])

    def along(c):
        whole = fb.at[c, pl.ds(0, kc - 16)]
        pltpu.make_async_copy(whole, whole, a2a_r.at[c]).wait()
        at_row = slice(c * kc, (c + 1) * kc)
        signed_rows(fb[c], tb[at_row, half:], lhs)
        width = half // BLOCKS
        for k in range(BLOCKS):
            at = slice(k * width, (k + 1) * width)
            part = jnp.dot(lhs[...], tb[at_row, at], preferred_element_type=F32)
            total = part if c == 0 else acc[:, at] + part
            if c < last - 1:
                acc[:, at] = total
            else:
                accb[:, at] = total.astype(BF16)

    stage(0)
    stage(1)
    far(0)
    stage(3)
    far(1)
    stage(8)
    relay(0)
    near(1)
    stage(4)
    stage(5)
    for cp in small[3:]:
        cp.wait()
    mcol[...] = jnp.transpose(jnp.broadcast_to(wave_v[...].reshape(1, mn).astype(F32), (8, mn)))
    far(2)
    stage(9)
    stage(6)
    relay(1)
    near(2)
    selection()
    swap(8).wait_recv()
    swap(9).wait_recv()
    early(0)
    stage(7)
    early(1)
    far(3)
    early(2)
    relay(2)
    near(3)
    finish(0)
    early(3)
    late_far()
    finish(1)
    relay(3)
    late_near()
    table(0)
    finish(2)
    table(1)
    late_relay()
    along(0)
    finish(3)
    table(4)
    send_table().start()
    table(2)
    table(3)
    along(1)
    along(2)
    late_finish()
    along(3)
    send_acc().start()

    for u in range(2 * nc):
        swap(u).wait_send()
    for u in ORDER[-DEPTH:]:
        for cp in keep(u):
            cp.wait()
    for kind in range(6):
        for c in range(last):
            hop(c, kind).wait_send()
        late_hop(kind).wait_send()
    send_table().wait()
    send_acc().wait()
    send_rows().wait()
    for box, sem in ((gb, a2a_s), (gbs, a2a_s2)):
        n = box.shape[0]
        flat = box.reshape(n * 2 * ma_n, 16, box.shape[4]).at[pl.ds(0, n * (2 * ma_n - 1))]
        pltpu.make_async_copy(flat, flat, sem).wait()


def grid_kernel(f_h, t_h, acc_h, kept_h, new_h, out_h, f, t, acc, kept, lhs, obuf, in_sem, keep_sem, out_sem):
    ln, rb, width = out_h.shape
    half = width // 2
    xb = half // BLOCKS
    parts = kept_h.shape[0]

    first = [
        pltpu.make_async_copy(f_h, f, in_sem.at[0]),
        pltpu.make_async_copy(t_h, t, in_sem.at[1]),
        pltpu.make_async_copy(acc_h, acc, in_sem.at[2]),
    ]
    take = [
        pltpu.make_async_copy(kept_h.at[c], kept.at[c], keep_sem.at[0, c]) for c in range(parts)
    ]
    give = [
        pltpu.make_async_copy(kept.at[c], new_h.at[c], keep_sem.at[1, c]) for c in range(parts)
    ]

    def store(k):
        return [
            pltpu.make_async_copy(
                obuf.at[k, p],
                out_h.at[:, :, pl.ds(p * half + k * xb, xb)],
                out_sem.at[k, p],
            )
            for p in range(2)
        ]

    for cp in first[:2] + take[:2] + first[2:] + take[2:]:
        cp.start()
    first[0].wait()
    first[1].wait()
    signed_rows(f[...], t[:, half:], lhs)
    first[2].wait()
    for k in range(max(BLOCKS, parts)):
        if k < parts:
            take[k].wait()
            give[k].start()
        if k < BLOCKS:
            at = slice(k * xb, (k + 1) * xb)
            part = jnp.dot(lhs[...], t[:, at], preferred_element_type=F32)
            part = (acc[:, at].astype(F32) + part).astype(BF16)
            for p in range(2):
                for level in range(ln):
                    r0 = (p * ln + level) * rb
                    obuf[k, p, level] = part[r0 : r0 + rb]
            for cp in store(k):
                cp.start()
    for k in range(BLOCKS):
        for cp in store(k):
            cp.wait()
    for cp in give:
        cp.wait()


def body(spectral_state, forcing_noise, decay_rate, amplitude, legendre, wave_of_slot, lat_of_row):
    ns, _, levels, wn = spectral_state.shape
    jn = legendre.shape[2]
    nlat = lat_of_row.shape[0]
    mn = wave_of_slot.shape[0]
    ma_n = mn // ns
    lev_n = lax.axis_size("lev")
    zn = lev_n // 2
    ln = levels // lev_n
    rb = nlat // ma_n
    nc = ns // S
    kn = 2 * mn
    kc = kn // nc
    half = NLON // 2
    lanes = -(-(ln * rb) // 128) * 128

    smem = pl.BlockSpec(memory_space=pltpu.SMEM)
    vmem = pl.BlockSpec(memory_space=pltpu.VMEM)
    hbm = pl.BlockSpec(memory_space=pl.ANY)
    box = pltpu.VMEM(((nc - 1) * Q, 32, jn), BF16)
    dma = pltpu.SemaphoreType.DMA
    f, t, acc, kept = pl.pallas_call(
        transform_kernel,
        out_shape=(
            jax.ShapeDtypeStruct((kc, lanes), BF16),
            jax.ShapeDtypeStruct((kc, half + RP), BF16),
            jax.ShapeDtypeStruct((2 * ln * rb, half), BF16),
            jax.ShapeDtypeStruct((nc, 2, 2, Q, 2, levels, wn), F32),
        ),
        in_specs=[hbm] * 7,
        out_specs=(hbm,) * 4,
        scratch_shapes=[
            pltpu.SMEM((mn,), jnp.int32),
            pltpu.VMEM((mn,), jnp.int32),
            pltpu.VMEM((nlat,), jnp.int32),
            pltpu.VMEM((levels,), F32),
            pltpu.VMEM((wn,), F32),
            pltpu.VMEM((DEPTH, 2, Q, 2, levels, wn), F32),
            pltpu.VMEM((DEPTH, 2, Q, 2, levels, wn), BF16),
            pltpu.VMEM((DEPTH, 2, Q, 2, levels, wn), F32),
            pltpu.VMEM((DEPTH, 2, Q, wn, jn), BF16),
            pltpu.VMEM((zn, ns, 32, jn), BF16),
            pltpu.VMEM((zn, ns // 2, 32, jn), BF16),
            box, box, box, box, box, box,
            pltpu.VMEM((128, 128), BF16),
            pltpu.VMEM((128, 2 * jn), BF16),
            pltpu.VMEM((128, 2 * jn), BF16),
            pltpu.VMEM((ma_n // 2, 2 * jn, 2 * RP), BF16),
            pltpu.VMEM((nc - 1, 2, ma_n, 16, lanes), BF16),
            pltpu.VMEM((4, 2, ma_n, 16, lanes), BF16),
            pltpu.VMEM((nc - 1, kc, lanes), BF16),
            pltpu.VMEM((4, kc, lanes), BF16),
            pltpu.VMEM((6, kc // 2, lanes), BF16),
            pltpu.VMEM((kn, half + RP), BF16),
            pltpu.VMEM((mn, 8), F32),
            pltpu.VMEM((ma_n // 2, 1, 2 * RP), jnp.int32),
            pltpu.VMEM((2 * ln * rb, half), F32),
            pltpu.VMEM((2 * ln * rb, half), BF16),
            pltpu.VMEM((2 * ln * rb, kc), BF16),
            dma((5,)),
            dma((DEPTH, 2)),
            dma((DEPTH, 2, 3)),
            dma((2 * nc,)),
            dma((2 * nc,)),
            dma((nc, 6)),
            dma((nc, 6)),
            dma,
            dma,
            dma((nc + 3,)),
            dma((3,)),
        ],
        compiler_params=pltpu.CompilerParams(
            collective_id=0, has_side_effects=True, vmem_limit_bytes=66_000_000
        ),
        name="transform",
    )(
        wave_of_slot, lat_of_row, decay_rate, amplitude,
        spectral_state.reshape(nc, 2, 2, Q, 2, levels, wn),
        forcing_noise.reshape(nc, 2, 2, Q, 2, levels, wn),
        legendre.reshape(nc, 2, 2, Q, wn, jn),
    )

    xb = half // BLOCKS
    new_state, pattern = pl.pallas_call(
        grid_kernel,
        out_shape=(
            jax.ShapeDtypeStruct((nc, S, 2, levels, wn), F32),
            jax.ShapeDtypeStruct((ln, rb, NLON), BF16),
        ),
        in_specs=[hbm] * 4,
        out_specs=(hbm, hbm),
        scratch_shapes=[
            pltpu.VMEM((kc, lanes), BF16),
            pltpu.VMEM((kc, half + RP), BF16),
            pltpu.VMEM((2 * ln * rb, half), BF16),
            pltpu.VMEM((nc, S, 2, levels, wn), F32),
            pltpu.VMEM((2 * ln * rb, kc), BF16),
            pltpu.VMEM((BLOCKS, 2, ln, rb, xb), BF16),
            dma((3,)),
            dma((2, nc)),
            dma((BLOCKS, 2)),
        ],
        compiler_params=pltpu.CompilerParams(vmem_limit_bytes=60_000_000),
        name="grid_rows",
    )(f, t, acc, kept.reshape(nc, S, 2, levels, wn))
    return (new_state.reshape(ns, 2, levels, wn), pattern)


def solution(mesh):
    return jax.shard_map(
        body,
        mesh=mesh,
        in_specs=(
            P("ma", None, None, "lev"),
            P("ma", None, None, "lev"),
            P(),
            P("lev"),
            P("ma", "lev", None),
            P(),
            P(),
        ),
        out_specs=(P("ma", None, None, "lev"), P("lev", "ma", None)),
        check_vma=False,
    )
```
